32 devices in a mesh: clients: 8 (over z, x), shard: 4 (over y, core).
Axes of the slice: x: 2, y: 2, z: 4, core: 2. Of those that a mesh axis runs over, the one named last changes fastest.
Arguments:
- quantized: int32 [8, 2097152], P('clients', 'shard'), may hold values from 0 to 2097151
- pair_masks: int32 [8, 2097152], P('clients', 'shard'), may hold values from 0 to 2097142, as said below
- alive_flags: int32 [8], P('clients'), may hold values from 0 to 1, as said below
- row_seeds: int32 [64], replicated, may hold values from 0 to 1073741823
Outputs:
- aggregate: int32 [2097152], P('shard')
- commitments: int32 [8, 64], P('clients')
- mismatch: int32 [64], replicated
The draws below stay inside these ranges and needn't reach their ends.
Inputs may be any that keep to these rules, and one draw needn't show every extreme that they name: For every position, the pair_masks of all 8 participants sum to a multiple of 2097143. `alive_flags`: at least one participant has flag 1 and at least one has flag 0.
All inputs are finite; a program needn't handle non-finite values.
Results may differ from the reference program's by a relative error of at most 0.000001.
Values may be sent and summed in bfloat16 or wider, within the bound.
A program may use at most 64 MiB of HBM per device.

```python
import math
import jax
import jax.numpy as jnp
from jax import lax

ROWS = 64
CLIENTS = 8
L = 2097152


def draw_pair_masks(key, part):
    drawn_base = jax.random.randint(jax.random.fold_in(key, 11), (CLIENTS, L), 0, 2097143, dtype=jnp.int32)
    following = jnp.roll(drawn_base, -1, axis=0)
    return (drawn_base - following) % 2097143


def draw_alive_flags(key, part):
    drawn_bits = jax.random.randint(jax.random.fold_in(key, 23), (CLIENTS,), 0, 2, dtype=jnp.int32)
    chosen = jax.random.randint(jax.random.fold_in(key, 29), (), 0, CLIENTS, dtype=jnp.int32)
    position = jnp.arange(CLIENTS, dtype=jnp.int32)
    drawn_bits = jnp.where(position == chosen, 0, drawn_bits)
    return jnp.where(position == (chosen + 1) % CLIENTS, 1, drawn_bits).astype(jnp.int32)


def with_ends(values, rng, least, largest):
    longest = values.shape.index(max(values.shape))
    spots = []
    for shift in (0, 1):
        where = [jax.random.randint(jax.random.fold_in(rng, axis), (), 0, length) for axis, length in enumerate(values.shape)]
        where[longest] = (where[longest] + shift) % values.shape[longest]
        spots.append(tuple(where))
    return values.at[spots[0]].set(least).at[spots[1]].set(largest)


def setup_inputs(seed: int = 0) -> dict:
    seeds = jax.random.split(jax.random.key(seed), 5)
    quantized = with_ends(jax.random.randint(seeds[0], (CLIENTS, L), 0, 2097152), jax.random.fold_in(seeds[0], 1), 0, 2097151).astype(jnp.int32)
    pair_masks = draw_pair_masks(jax.random.fold_in(seeds[4], 71), 0)
    alive_flags = draw_alive_flags(jax.random.fold_in(seeds[4], 71), 0)
    row_seeds = with_ends(jax.random.randint(seeds[3], (ROWS,), 0, 1073741824), jax.random.fold_in(seeds[3], 1), 0, 1073741823).astype(jnp.int32)
    return dict(quantized=quantized, pair_masks=pair_masks, alive_flags=alive_flags, row_seeds=row_seeds)


modulus = 2097143


def table_entries(row_seeds, columns):
    mixed = columns[None, :] * 747796405 + row_seeds[:, None]
    mixed = mixed & 2147483647
    mixed = mixed ^ (mixed >> 15)
    mixed = (mixed * 277803737) & 2147483647
    mixed = mixed ^ (mixed >> 13)
    mixed = (mixed * 1103515245) & 2147483647
    mixed = mixed ^ (mixed >> 16)
    return mixed & 1023


def project_mod(row_seeds, vectors, offset, block_width):
    vec_count = vectors.shape[0]
    length = vectors.shape[1]
    row_count = row_seeds.shape[0]
    sub_width = math.gcd(block_width, 512)
    block_count = length // block_width

    def advance(running, block_index):
        start_col = block_index * block_width
        columns = offset + start_col + jnp.arange(block_width, dtype=jnp.int32)
        table = table_entries(row_seeds, columns)
        right_part = lax.dynamic_slice_in_dim(vectors, start_col, block_width, 1)
        products = (right_part[:, None, :] * table[None, :, :]) % modulus
        products = products.reshape(vec_count, row_count, block_width // sub_width, sub_width)
        partial_value = jnp.sum(products, axis=3, dtype=jnp.int32) % modulus
        partial_value = jnp.sum(partial_value, axis=2, dtype=jnp.int32) % modulus
        return (running + partial_value) % modulus, None

    running = jnp.zeros((vec_count, row_count), jnp.int32)
    running, unused = lax.scan(advance, running, jnp.arange(block_count, dtype=jnp.int32))
    return running


def reference(quantized, pair_masks, alive_flags, row_seeds):
    masked = ((quantized + pair_masks) % modulus) * alive_flags[:, None]
    aggregate = jnp.sum(masked, axis=0, dtype=jnp.int32) % modulus
    col_block = math.gcd(quantized.shape[1], 4096)
    commitments = project_mod(row_seeds, quantized, 0, col_block)
    expected = jnp.sum(commitments * alive_flags[:, None], axis=0, dtype=jnp.int32) % modulus
    projected = project_mod(row_seeds, aggregate[None, :], 0, col_block)[0]
    mismatch = (projected - expected) % modulus
    return aggregate, commitments, mismatch
```

```python
import functools
import math

import jax
import jax.numpy as jnp
from jax import lax
from jax.experimental import pallas as pl
from jax.experimental.pallas import tpu as pltpu
from jax.sharding import PartitionSpec as P

modulus = 2097143
LANES = 128


def reduce_mod(x):
    x = (x & 2097151) + (x >> 21) * 9
    return jnp.where(x >= modulus, x - modulus, x)


def table_tile(start):
    v = start & 2147483647
    v = v ^ (v >> 15)
    v = (v * 277803737) & 2147483647
    v = v ^ (v >> 13)
    v = v * 1103515245
    v = v ^ (v >> 16)
    high = (v & 992).astype(jnp.float32).astype(jnp.bfloat16)
    low = (v & 31).astype(jnp.float32).astype(jnp.bfloat16)
    return high, low


def project_kernel(block, group, start_ref, seeds_ref, *refs):
    count = (len(refs) - 3) // 1
    vec_refs = refs[:count]
    out_ref, table_ref, base_ref = refs[count:]
    step = pl.program_id(0)
    rows = seeds_ref.shape[0]

    @pl.when(step == 0)
    def _():
        lane = lax.broadcasted_iota(jnp.int32, (rows, LANES), 1)
        base_ref[...] = (lane + start_ref[0]) * 747796405 + seeds_ref[...]
        out_ref[...] = jnp.zeros_like(out_ref)

    width = 8 * ((3 * count + 7) // 8)
    sub = lax.broadcasted_iota(jnp.int32, (width, group), 0)
    base = base_ref[...]
    total = None
    for g in range(block // group):
        for k in range(group // LANES):
            first = (step * block + (g * group + k * LANES)) * 747796405
            high, low = table_tile(base + first)
            cols = pl.ds(k * LANES, LANES)
            table_ref[g, :rows, cols] = high
            table_ref[g, rows:, cols] = low
        picked = None
        for n in range(count):
            one = jnp.broadcast_to(vec_refs[n][:, g * group : (g + 1) * group], (width, group))
            picked = one if picked is None else jnp.where(sub >= 3 * n, one, picked)
        shift = 7 * (sub % 3)
        pieces = ((picked >> shift) & 127).astype(jnp.float32).astype(jnp.bfloat16)
        part = lax.dot_general(
            table_ref[g], pieces, (((1,), (1,)), ((), ())), preferred_element_type=jnp.float32
        )
        total = part if total is None else total + part
    total = total.astype(jnp.int32)
    out_ref[...] = reduce_mod(out_ref[...] + total)


def project(row_seeds, vectors, start, block=4096, group=1024):
    rows = row_seeds.shape[0]
    length = vectors[0].shape[1]
    block = math.gcd(length, block)
    group = math.gcd(block, group)
    count = len(vectors)
    width = 8 * ((3 * count + 7) // 8)
    parts = pl.pallas_call(
        functools.partial(project_kernel, block, group),
        grid=(length // block,),
        in_specs=[
            pl.BlockSpec(memory_space=pltpu.SMEM),
            pl.BlockSpec((rows, 1), lambda i: (0, 0)),
        ]
        + [pl.BlockSpec((1, block), lambda i: (0, i))] * count,
        out_specs=pl.BlockSpec((2 * rows, width), lambda i: (0, 0)),
        out_shape=jax.ShapeDtypeStruct((2 * rows, width), jnp.int32),
        scratch_shapes=[
            pltpu.VMEM((block // group, 2 * rows, group), jnp.bfloat16),
            pltpu.VMEM((rows, LANES), jnp.int32),
        ],
        cost_estimate=pl.CostEstimate(
            flops=length * rows * 60, bytes_accessed=length * 4 * count, transcendentals=0
        ),
        name="project",
    )(start.reshape(1), row_seeds[:, None], *vectors)
    both = reduce_mod(parts[:rows] + parts[rows:])
    out = []
    for n in range(count):
        value = both[:, 3 * n + 2]
        value = reduce_mod(value * 128 + both[:, 3 * n + 1])
        value = reduce_mod(value * 128 + both[:, 3 * n])
        out.append(value)
    return out


def body(quantized, pair_masks, alive_flags, row_seeds):
    alive_now = alive_flags[0]
    length = quantized.shape[1]
    clients = lax.axis_size("clients")
    client = lax.axis_index("clients")
    rows = row_seeds.shape[0]
    masked = quantized + pair_masks
    masked = jnp.where(masked >= modulus, masked - modulus, masked)
    masked = jnp.where(masked >= modulus, masked - modulus, masked) * alive_now
    summed = lax.psum(masked[0], "clients")
    aggregate = reduce_mod(summed)
    offset = lax.axis_index("shard") * length
    own, arrived = project(row_seeds, [quantized, masked], offset)
    mine = jnp.arange(clients, dtype=jnp.int32)[:, None] == client
    left = jnp.where(mine, own[None, :], 0)
    diff = (arrived - own * alive_now)
    diff = jnp.where(diff < 0, diff + modulus, diff)
    both = lax.psum(jnp.concatenate([left, diff[None, :]], 0), ("clients", "shard"))
    commitments = reduce_mod(lax.dynamic_slice_in_dim(both, client, 1, 0))
    mismatch = reduce_mod(both[clients])
    return (aggregate, commitments, mismatch)


def solution(mesh):
    placed = (P("clients", "shard"), P("clients", "shard"), P("clients"), P())
    return jax.shard_map(
        body,
        mesh=mesh,
        in_specs=placed,
        out_specs=(P("shard"), P("clients", None), P()),
        check_vma=False,
    )
```

```python
import functools

import jax
import jax.numpy as jnp
from jax import lax
from jax.experimental import pallas as pl
from jax.experimental.pallas import tpu as pltpu
from jax.sharding import PartitionSpec as P

modulus = 2097143
LANES = 128
GROUP = 16
STRIDE = (LANES * 747796405 + 2147483648) % 4294967296 - 2147483648


def reduce_mod(x):
    x = (x & 2097151) + (x >> 21) * 9
    return jnp.where(x >= modulus, x - modulus, x)


def table_tile(start):
    v = start & 2147483647
    v = v ^ (v >> 15)
    v = (v * 277803737) & 2147483647
    v = v ^ (v >> 13)
    v = v * 1103515245
    v = v ^ (v >> 16)
    high = (v & 992).astype(jnp.float32).astype(jnp.bfloat16)
    low = (v & 31).astype(jnp.float32).astype(jnp.bfloat16)
    return high, low


def aggregate_kernel(
    clients,
    length,
    alive_ref,
    seeds_ref,
    quant_ref,
    masks_ref,
    agg_out,
    proj_out,
    masked,
    arrived,
    agg,
    base,
    tables,
    pieces,
    send_sem,
    recv_sem,
    out_sem,
):
    rows = quant_ref.shape[0]
    half = rows // 2
    checks = seeds_ref.shape[0]
    bits = clients.bit_length() - 1
    me = lax.axis_index("clients")
    start = lax.axis_index("shard") * length
    alive = alive_ref[0]

    barrier = pltpu.get_barrier_semaphore()
    for b in range(bits):
        pl.semaphore_signal(barrier, inc=1, device_id={"clients": me ^ (1 << b)})

    def mask_rows(lo, count):
        step = min(64, count)

        @pl.loop(0, count // step)
        def _(i):
            at = pl.ds(pl.multiple_of(lo + i * step, 8), step)
            s = quant_ref[at, :] + masks_ref[at, :]
            s = jnp.where(s >= modulus, s - modulus, s)
            s = jnp.where(s >= modulus, s - modulus, s)
            masked[at, :] = s * alive

    plans = []
    for h in range(2):
        order = list(range(bits))
        if h == 1:
            order = order[1:] + order[:1]
        lo = h * half
        count = half
        landing = h * half
        scatter, gather = [], []
        for n, b in enumerate(order):
            count //= 2
            bit = (me >> b) & 1
            keep = pl.multiple_of(lo + bit * count, 8)
            give = pl.multiple_of(lo + (1 - bit) * count, 8)
            scatter.append((b, keep, give, count, landing, n))
            gather.append((b, keep, give, count, n))
            landing += count
            lo = keep
        plans.append((scatter, gather[::-1], lo, count))

    def scatter_copy(h, n):
        b, keep, give, count, landing, _ = plans[h][0][n]
        return pltpu.make_async_remote_copy(
            src_ref=masked.at[pl.ds(give, count)],
            dst_ref=arrived.at[pl.ds(landing, count)],
            send_sem=send_sem.at[h, n],
            recv_sem=recv_sem.at[h, n],
            device_id={"clients": me ^ (1 << b)},
        )

    def gather_copy(h, n):
        b, keep, give, count, _ = plans[h][1][n]
        return pltpu.make_async_remote_copy(
            src_ref=agg.at[pl.ds(keep, count)],
            dst_ref=agg.at[pl.ds(keep, count)],
            send_sem=send_sem.at[h, bits + n],
            recv_sem=recv_sem.at[h, bits + n],
            device_id={"clients": me ^ (1 << b)},
        )

    def gather_wait(h, n):
        b, keep, give, count, _ = plans[h][1][n]
        gather_copy(h, n).wait_send()
        pltpu.make_async_remote_copy(
            src_ref=agg.at[pl.ds(give, count)],
            dst_ref=agg.at[pl.ds(give, count)],
            send_sem=send_sem.at[h, bits + n],
            recv_sem=recv_sem.at[h, bits + n],
            device_id={"clients": me ^ (1 << b)},
        ).wait_recv()

    def add_arrived(h, n):
        _, keep, _, count, landing, _ = plans[h][0][n]
        step = min(64, count)
        last = n == bits - 1

        @pl.loop(0, count // step)
        def _(i):
            at = pl.ds(pl.multiple_of(keep + i * step, 8), step)
            got = pl.ds(pl.multiple_of(landing + i * step, 8), step)
            s = masked[at, :] + arrived[got, :]
            if last:
                agg[at, :] = reduce_mod(s)
            else:
                masked[at, :] = s

    for h in range(2):
        _, keep, give, count, _, _ = plans[h][0][0]
        mask_rows(give, count)
    lane = lax.broadcasted_iota(jnp.int32, (checks, LANES), 1)
    base[...] = (lane + start) * 747796405 + seeds_ref[...]
    tables[1] = jnp.zeros_like(tables[1])
    pieces[1] = jnp.zeros_like(pieces[1])
    pl.semaphore_wait(barrier, bits)
    for h in range(2):
        scatter_copy(h, 0).start()
    for h in range(2):
        _, keep, give, count, _, _ = plans[h][0][0]
        mask_rows(keep, count)

    sub = lax.broadcasted_iota(jnp.int32, (8, LANES), 0)
    shift = 7 * (sub & 3)
    second = sub >= 4

    def pending(slot, total):
        part = lax.dot_general(
            pieces[slot], tables[slot], (((1,), (1,)), ((), ())), preferred_element_type=jnp.float32
        )
        return reduce_mod(total + part.astype(jnp.int32))

    def fill(slot, row):
        for k in range(GROUP):
            at = row + k
            high, low = table_tile(base[...] + at * STRIDE)
            cols = pl.ds(k * LANES, LANES)
            tables[slot, :checks, cols] = high
            tables[slot, checks:, cols] = low
            one = jnp.broadcast_to(quant_ref[pl.ds(at, 1), :], (8, LANES))
            two = jnp.broadcast_to(masked_row(at), (8, LANES))
            both = (jnp.where(second, two, one) >> shift) & 127
            pieces[slot, :, cols] = both.astype(jnp.float32).astype(jnp.bfloat16)

    def masked_row(at):
        s = quant_ref[pl.ds(at, 1), :] + masks_ref[pl.ds(at, 1), :]
        s = jnp.where(s >= modulus, s - modulus, s)
        return jnp.where(s >= modulus, s - modulus, s) * alive

    def compute(first, count, total):
        def pair(i, total):
            row = first + i * (2 * GROUP)
            total = pending(1, total)
            fill(0, row)
            total = pending(0, total)
            fill(1, row + GROUP)
            return total

        return lax.fori_loop(0, count, pair, total)

    actions = []
    for n in range(bits):
        for h in range(2):
            def take(h=h, n=n):
                scatter_copy(h, n).wait()
                add_arrived(h, n)

            def send(h=h, n=n):
                if n < bits - 1:
                    scatter_copy(h, n + 1).start()
                else:
                    gather_copy(h, 0).start()

            actions.append((take, send))
    for n in range(bits):
        for h in range(2):
            def take(h=h, n=n):
                gather_wait(h, n)

            def send(h=h, n=n):
                if n < bits - 1:
                    gather_copy(h, n + 1).start()

            actions.append((take, send))

    pairs = rows // (2 * GROUP)
    stops = len(actions) + 1
    done = 0
    total = jnp.zeros((8, LANES), jnp.int32)
    for s, (take, send) in enumerate(actions):
        until = pairs * (s + 1) // stops
        total = compute(done * 2 * GROUP, until - done, total)
        done = until
        take()
        send()
    store = pltpu.make_async_copy(agg, agg_out, out_sem)
    store.start()
    total = compute(done * 2 * GROUP, pairs - done, total)
    proj_out[...] = pending(1, total)
    store.wait()


def aggregate_and_project(quantized, pair_masks, alive_flags, row_seeds, clients):
    length = quantized.shape[1]
    rows = length // LANES
    checks = row_seeds.shape[0]
    bits = clients.bit_length() - 1
    vmem = pl.BlockSpec(memory_space=pltpu.VMEM)
    return pl.pallas_call(
        functools.partial(aggregate_kernel, clients, length),
        in_specs=[pl.BlockSpec(memory_space=pltpu.SMEM), vmem, vmem, vmem],
        out_specs=[pl.BlockSpec(memory_space=pl.ANY), vmem],
        out_shape=[
            jax.ShapeDtypeStruct((rows, LANES), jnp.int32),
            jax.ShapeDtypeStruct((8, 2 * checks), jnp.int32),
        ],
        scratch_shapes=[
            pltpu.VMEM((rows, LANES), jnp.int32),
            pltpu.VMEM((rows, LANES), jnp.int32),
            pltpu.VMEM((rows, LANES), jnp.int32),
            pltpu.VMEM((checks, LANES), jnp.int32),
            pltpu.VMEM((2, 2 * checks, GROUP * LANES), jnp.bfloat16),
            pltpu.VMEM((2, 8, GROUP * LANES), jnp.bfloat16),
            pltpu.SemaphoreType.DMA((2, 2 * bits)),
            pltpu.SemaphoreType.DMA((2, 2 * bits)),
            pltpu.SemaphoreType.DMA,
        ],
        compiler_params=pltpu.CompilerParams(collective_id=0, has_side_effects=True),
        name="aggregate_and_project",
    )(
        alive_flags,
        row_seeds[:, None],
        quantized.reshape(rows, LANES),
        pair_masks.reshape(rows, LANES),
    )


def body(quantized, pair_masks, alive_flags, row_seeds):
    alive_now = alive_flags[0]
    length = quantized.shape[1]
    clients = lax.axis_size("clients")
    client = lax.axis_index("clients")
    checks = row_seeds.shape[0]
    aggregate, parts = aggregate_and_project(
        quantized, pair_masks, alive_flags, row_seeds, clients
    )
    parts = reduce_mod(parts[:, :checks] + parts[:, checks:])
    own, arrived = [
        reduce_mod(reduce_mod(parts[n + 2] * 128 + parts[n + 1]) * 128 + parts[n]) for n in (0, 4)
    ]
    mine = jnp.arange(clients, dtype=jnp.int32)[:, None] == client
    left = jnp.where(mine, own[None, :], 0)
    diff = arrived - own * alive_now
    diff = jnp.where(diff < 0, diff + modulus, diff)
    both = lax.psum(jnp.concatenate([left, diff[None, :]], 0), ("clients", "shard"))
    commitments = reduce_mod(lax.dynamic_slice_in_dim(both, client, 1, 0))
    mismatch = reduce_mod(both[clients])
    return (aggregate.reshape(length), commitments, mismatch)


def solution(mesh):
    placed = (P("clients", "shard"), P("clients", "shard"), P("clients"), P())
    return jax.shard_map(
        body,
        mesh=mesh,
        in_specs=placed,
        out_specs=(P("shard"), P("clients", None), P()),
        check_vma=False,
    )
```

```python
import functools

import jax
import jax.numpy as jnp
from jax import lax
from jax.experimental import pallas as pl
from jax.experimental.pallas import tpu as pltpu
from jax.sharding import PartitionSpec as P

modulus = 2097143
LANES = 128
GROUP = 16
STRIDE = (LANES * 747796405 + 2147483648) % 4294967296 - 2147483648


def reduce_mod(x):
    x = (x & 2097151) + (x >> 21) * 9
    return jnp.where(x >= modulus, x - modulus, x)


def table_tile(start):
    v = start & 2147483647
    v = v ^ (v >> 15)
    v = (v * 277803737) & 2147483647
    v = v ^ (v >> 13)
    v = v * 1103515245
    v = v ^ (v >> 16)
    high = (v & 992).astype(jnp.float32).astype(jnp.bfloat16)
    low = (v & 31).astype(jnp.float32).astype(jnp.bfloat16)
    return high, low


def aggregate_kernel(
    clients,
    length,
    alive_ref,
    seeds_ref,
    quant_ref,
    masks_ref,
    agg_out,
    own_out,
    diff_out,
    masked,
    arrived,
    agg,
    base,
    tables,
    pieces,
    send_sem,
    recv_sem,
    out_sem,
    own_parts,
    diff_parts,
    own_send,
    own_recv,
    diff_send,
    diff_recv,
):
    rows = quant_ref.shape[0]
    half = rows // 2
    checks = seeds_ref.shape[0]
    bits = clients.bit_length() - 1
    me = lax.axis_index("clients")
    shards = lax.axis_size("shard")
    here = lax.axis_index("shard")
    start = lax.axis_index("shard") * length
    alive = alive_ref[0]

    barrier = pltpu.get_barrier_semaphore()
    for n in range(1, clients):
        pl.semaphore_signal(barrier, inc=1, device_id={"clients": me ^ n})
    for n in range(1, shards):
        pl.semaphore_signal(barrier, inc=1, device_id={"shard": lax.rem(here + n, shards)})

    def mask_rows(lo, count):
        step = min(64, count)

        @pl.loop(0, count // step)
        def _(i):
            at = pl.ds(pl.multiple_of(lo + i * step, 8), step)
            s = quant_ref[at, :] + masks_ref[at, :]
            s = jnp.where(s >= modulus, s - modulus, s)
            s = jnp.where(s >= modulus, s - modulus, s)
            masked[at, :] = s * alive

    plans = []
    for h in range(2):
        order = list(range(bits))
        if h == 1:
            order = order[1:] + order[:1]
        lo = h * half
        count = half
        landing = h * half
        scatter, gather = [], []
        for n, b in enumerate(order):
            count //= 2
            bit = (me >> b) & 1
            keep = pl.multiple_of(lo + bit * count, 8)
            give = pl.multiple_of(lo + (1 - bit) * count, 8)
            scatter.append((b, keep, give, count, landing, n))
            gather.append((b, keep, give, count, n))
            landing += count
            lo = keep
        plans.append((scatter, gather[::-1], lo, count))

    def scatter_copy(h, n):
        b, keep, give, count, landing, _ = plans[h][0][n]
        return pltpu.make_async_remote_copy(
            src_ref=masked.at[pl.ds(give, count)],
            dst_ref=arrived.at[pl.ds(landing, count)],
            send_sem=send_sem.at[h, n],
            recv_sem=recv_sem.at[h, n],
            device_id={"clients": me ^ (1 << b)},
        )

    def gather_copy(h, n):
        b, keep, give, count, _ = plans[h][1][n]
        return pltpu.make_async_remote_copy(
            src_ref=agg.at[pl.ds(keep, count)],
            dst_ref=agg.at[pl.ds(keep, count)],
            send_sem=send_sem.at[h, bits + n],
            recv_sem=recv_sem.at[h, bits + n],
            device_id={"clients": me ^ (1 << b)},
        )

    def gather_wait(h, n):
        b, keep, give, count, _ = plans[h][1][n]
        gather_copy(h, n).wait_send()
        pltpu.make_async_remote_copy(
            src_ref=agg.at[pl.ds(give, count)],
            dst_ref=agg.at[pl.ds(give, count)],
            send_sem=send_sem.at[h, bits + n],
            recv_sem=recv_sem.at[h, bits + n],
            device_id={"clients": me ^ (1 << b)},
        ).wait_recv()

    def add_arrived(h, n):
        _, keep, _, count, landing, _ = plans[h][0][n]
        step = min(64, count)
        last = n == bits - 1

        @pl.loop(0, count // step)
        def _(i):
            at = pl.ds(pl.multiple_of(keep + i * step, 8), step)
            got = pl.ds(pl.multiple_of(landing + i * step, 8), step)
            s = masked[at, :] + arrived[got, :]
            if last:
                agg[at, :] = reduce_mod(s)
            else:
                masked[at, :] = s

    for h in range(2):
        _, keep, give, count, _, _ = plans[h][0][0]
        mask_rows(give, count)
    lane = lax.broadcasted_iota(jnp.int32, (checks, LANES), 1)
    base[...] = (lane + start) * 747796405 + seeds_ref[...]
    tables[1] = jnp.zeros_like(tables[1])
    pieces[1] = jnp.zeros_like(pieces[1])
    pl.semaphore_wait(barrier, clients + shards - 2)
    for h in range(2):
        scatter_copy(h, 0).start()
    for h in range(2):
        _, keep, give, count, _, _ = plans[h][0][0]
        mask_rows(keep, count)

    sub = lax.broadcasted_iota(jnp.int32, (8, LANES), 0)
    shift = 7 * (sub & 3)
    second = sub >= 4

    def pending(slot, total):
        part = lax.dot_general(
            pieces[slot], tables[slot], (((1,), (1,)), ((), ())), preferred_element_type=jnp.float32
        )
        return reduce_mod(total + part.astype(jnp.int32))

    def fill(slot, row):
        for k in range(GROUP):
            at = row + k
            high, low = table_tile(base[...] + at * STRIDE)
            cols = pl.ds(k * LANES, LANES)
            tables[slot, :checks, cols] = high
            tables[slot, checks:, cols] = low
            one = jnp.broadcast_to(quant_ref[pl.ds(at, 1), :], (8, LANES))
            two = jnp.broadcast_to(masked_row(at), (8, LANES))
            both = (jnp.where(second, two, one) >> shift) & 127
            pieces[slot, :, cols] = both.astype(jnp.float32).astype(jnp.bfloat16)

    def masked_row(at):
        s = quant_ref[pl.ds(at, 1), :] + masks_ref[pl.ds(at, 1), :]
        s = jnp.where(s >= modulus, s - modulus, s)
        return jnp.where(s >= modulus, s - modulus, s) * alive

    def compute(first, count, total):
        def pair(i, total):
            row = first + i * (2 * GROUP)
            total = pending(1, total)
            fill(0, row)
            total = pending(0, total)
            fill(1, row + GROUP)
            return total

        return lax.fori_loop(0, count, pair, total)

    actions = []
    for n in range(bits):
        for h in range(2):
            def take(h=h, n=n):
                scatter_copy(h, n).wait()
                add_arrived(h, n)

            def send(h=h, n=n):
                if n < bits - 1:
                    scatter_copy(h, n + 1).start()
                else:
                    gather_copy(h, 0).start()

            actions.append((take, send))
    for n in range(bits):
        for h in range(2):
            def take(h=h, n=n):
                gather_wait(h, n)

            def send(h=h, n=n):
                if n < bits - 1:
                    gather_copy(h, n + 1).start()

            actions.append((take, send))

    pairs = rows // (2 * GROUP)
    stops = len(actions) + 1
    done = 0
    total = jnp.zeros((8, LANES), jnp.int32)
    for s, (take, send) in enumerate(actions):
        until = pairs * (s + 1) // stops
        total = compute(done * 2 * GROUP, until - done, total)
        done = until
        take()
        send()
    store = pltpu.make_async_copy(agg, agg_out, out_sem)
    store.start()
    total = compute(done * 2 * GROUP, pairs - done, total)
    total = pending(1, total)

    own_parts[0] = total
    own_copies = [
        pltpu.make_async_remote_copy(
            src_ref=own_parts.at[0],
            dst_ref=own_parts.at[n],
            send_sem=own_send.at[n],
            recv_sem=own_recv.at[n],
            device_id={"shard": lax.rem(here + n, shards)},
        )
        for n in range(1, shards)
    ]
    for copy in own_copies:
        copy.start()
    for copy in own_copies:
        copy.wait()
    for n in range(1, shards):
        total = total + own_parts[n]
    total = reduce_mod(total)
    own_out[...] = total
    diff = pltpu.roll(total, 4, 0) - total * alive
    diff = jnp.where(diff < 0, diff + modulus, diff)
    diff_parts[0] = diff
    diff_copies = [
        pltpu.make_async_remote_copy(
            src_ref=diff_parts.at[0],
            dst_ref=diff_parts.at[n],
            send_sem=diff_send.at[n],
            recv_sem=diff_recv.at[n],
            device_id={"clients": me ^ n},
        )
        for n in range(1, clients)
    ]
    for copy in diff_copies:
        copy.start()
    for copy in diff_copies:
        copy.wait()
    for n in range(1, clients):
        diff = diff + diff_parts[n]
    diff_out[...] = reduce_mod(diff)
    store.wait()


def aggregate_and_project(quantized, pair_masks, alive_flags, row_seeds, clients, shards):
    length = quantized.shape[1]
    rows = length // LANES
    checks = row_seeds.shape[0]
    bits = clients.bit_length() - 1
    vmem = pl.BlockSpec(memory_space=pltpu.VMEM)
    return pl.pallas_call(
        functools.partial(aggregate_kernel, clients, length),
        in_specs=[pl.BlockSpec(memory_space=pltpu.SMEM), vmem, vmem, vmem],
        out_specs=[pl.BlockSpec(memory_space=pl.ANY), vmem, vmem],
        out_shape=[
            jax.ShapeDtypeStruct((rows, LANES), jnp.int32),
            jax.ShapeDtypeStruct((8, 2 * checks), jnp.int32),
            jax.ShapeDtypeStruct((8, 2 * checks), jnp.int32),
        ],
        scratch_shapes=[
            pltpu.VMEM((rows, LANES), jnp.int32),
            pltpu.VMEM((rows, LANES), jnp.int32),
            pltpu.VMEM((rows, LANES), jnp.int32),
            pltpu.VMEM((checks, LANES), jnp.int32),
            pltpu.VMEM((2, 2 * checks, GROUP * LANES), jnp.bfloat16),
            pltpu.VMEM((2, 8, GROUP * LANES), jnp.bfloat16),
            pltpu.SemaphoreType.DMA((2, 2 * bits)),
            pltpu.SemaphoreType.DMA((2, 2 * bits)),
            pltpu.SemaphoreType.DMA,
            pltpu.VMEM((shards, 8, 2 * checks), jnp.int32),
            pltpu.VMEM((clients, 8, 2 * checks), jnp.int32),
            pltpu.SemaphoreType.DMA((shards,)),
            pltpu.SemaphoreType.DMA((shards,)),
            pltpu.SemaphoreType.DMA((clients,)),
            pltpu.SemaphoreType.DMA((clients,)),
        ],
        compiler_params=pltpu.CompilerParams(collective_id=0, has_side_effects=True),
        name="aggregate_and_project",
    )(
        alive_flags,
        row_seeds[:, None],
        quantized.reshape(rows, LANES),
        pair_masks.reshape(rows, LANES),
    )


def checksum(parts):
    checks = parts.shape[1] // 2
    parts = reduce_mod(parts[:, :checks] + parts[:, checks:])
    return reduce_mod(reduce_mod(parts[2] * 128 + parts[1]) * 128 + parts[0])


def body(quantized, pair_masks, alive_flags, row_seeds):
    length = quantized.shape[1]
    clients = lax.axis_size("clients")
    shards = lax.axis_size("shard")
    aggregate, own, diff = aggregate_and_project(
        quantized, pair_masks, alive_flags, row_seeds, clients, shards
    )
    return (aggregate.reshape(length), checksum(own)[None, :], checksum(diff))


def solution(mesh):
    placed = (P("clients", "shard"), P("clients", "shard"), P("clients"), P())
    return jax.shard_map(
        body,
        mesh=mesh,
        in_specs=placed,
        out_specs=(P("shard"), P("clients", None), P()),
        check_vma=False,
    )
```

```python
import functools

import jax
import jax.numpy as jnp
from jax import lax
from jax.experimental import pallas as pl
from jax.experimental.pallas import tpu as pltpu
from jax.sharding import PartitionSpec as P

modulus = 2097143
LANES = 128
GROUP = 16
STRIDE = (LANES * 747796405 + 2147483648) % 4294967296 - 2147483648


def reduce_mod(x):
    x = (x & 2097151) + (x >> 21) * 9
    return jnp.where(x >= modulus, x - modulus, x)


def table_tile(start):
    v = start & 2147483647
    v = v ^ (v >> 15)
    v = (v * 277803737) & 2147483647
    v = v ^ (v >> 13)
    v = v * 1103515245
    v = v ^ (v >> 16)
    high = (v & 992).astype(jnp.float32).astype(jnp.bfloat16)
    low = (v & 31).astype(jnp.float32).astype(jnp.bfloat16)
    return high, low


def aggregate_kernel(
    clients,
    length,
    alive_ref,
    seeds_ref,
    quant_ref,
    masks_ref,
    agg_out,
    own_out,
    diff_out,
    masked,
    arrived,
    agg,
    base,
    tables,
    pieces,
    send_sem,
    recv_sem,
    out_sem,
    own_parts,
    diff_parts,
    own_send,
    own_recv,
    diff_send,
    diff_recv,
    partner_q,
    swap_send,
    swap_recv,
):
    rows = quant_ref.shape[0]
    half = rows // 2
    checks = seeds_ref.shape[0]
    bits = clients.bit_length() - 1
    me = lax.axis_index("clients")
    shards = lax.axis_size("shard")
    here = lax.axis_index("shard")
    start = lax.axis_index("shard") * length
    alive = alive_ref[0]

    barrier = pltpu.get_barrier_semaphore()
    for n in range(1, clients):
        pl.semaphore_signal(barrier, inc=1, device_id={"clients": me ^ n})
    for n in range(1, shards):
        there = lax.rem(here + n, shards)
        pl.semaphore_signal(barrier, inc=1, device_id={"shard": there})
        pl.semaphore_signal(barrier, inc=1, device_id={"shard": there, "clients": me ^ 1})
    peers = clients + 2 * shards - 3

    def mask_rows(lo, count):
        step = min(64, count)

        @pl.loop(0, count // step)
        def _(i):
            at = pl.ds(pl.multiple_of(lo + i * step, 8), step)
            s = quant_ref[at, :] + masks_ref[at, :]
            s = jnp.where(s >= modulus, s - modulus, s)
            s = jnp.where(s >= modulus, s - modulus, s)
            masked[at, :] = s * alive

    plans = []
    for h in range(2):
        order = list(range(bits))
        if h == 1:
            order = order[1:] + order[:1]
        lo = h * half
        count = half
        landing = h * half
        scatter, gather = [], []
        for n, b in enumerate(order):
            count //= 2
            bit = (me >> b) & 1
            keep = pl.multiple_of(lo + bit * count, 8)
            give = pl.multiple_of(lo + (1 - bit) * count, 8)
            scatter.append((b, keep, give, count, landing, n))
            gather.append((b, keep, give, count, n))
            landing += count
            lo = keep
        plans.append((scatter, gather[::-1], lo, count))

    def scatter_copy(h, n):
        b, keep, give, count, landing, _ = plans[h][0][n]
        return pltpu.make_async_remote_copy(
            src_ref=masked.at[pl.ds(give, count)],
            dst_ref=arrived.at[pl.ds(landing, count)],
            send_sem=send_sem.at[h, n],
            recv_sem=recv_sem.at[h, n],
            device_id={"clients": me ^ (1 << b)},
        )

    def gather_copy(h, n):
        b, keep, give, count, _ = plans[h][1][n]
        return pltpu.make_async_remote_copy(
            src_ref=agg.at[pl.ds(keep, count)],
            dst_ref=agg.at[pl.ds(keep, count)],
            send_sem=send_sem.at[h, bits + n],
            recv_sem=recv_sem.at[h, bits + n],
            device_id={"clients": me ^ (1 << b)},
        )

    def gather_wait(h, n):
        b, keep, give, count, _ = plans[h][1][n]
        gather_copy(h, n).wait_send()
        pltpu.make_async_remote_copy(
            src_ref=agg.at[pl.ds(give, count)],
            dst_ref=agg.at[pl.ds(give, count)],
            send_sem=send_sem.at[h, bits + n],
            recv_sem=recv_sem.at[h, bits + n],
            device_id={"clients": me ^ (1 << b)},
        ).wait_recv()

    def add_arrived(h, n):
        _, keep, _, count, landing, _ = plans[h][0][n]
        step = min(64, count)
        last = n == bits - 1

        @pl.loop(0, count // step)
        def _(i):
            at = pl.ds(pl.multiple_of(keep + i * step, 8), step)
            got = pl.ds(pl.multiple_of(landing + i * step, 8), step)
            s = masked[at, :] + arrived[got, :]
            if last:
                agg[at, :] = reduce_mod(s)
            else:
                masked[at, :] = s

    block = half // clients
    shares = [plans[0][2] // block, (plans[1][2] - half) // block]
    unit = 2 * GROUP
    per_block = block // unit
    others = clients // 2 - 1

    def block_row(h, k, flip=0):
        if h == 0:
            return (shares[0] ^ (k + flip * (clients // 2))) * block
        return half + (shares[1] ^ (2 * k + flip)) * block

    work = [(h, k) for h in range(2) for k in range(others, 0, -1)] + [(0, 0), (1, 0)]

    def swap_copy(n):
        at = pl.multiple_of(block_row(*work[n], 1), 8)
        return pltpu.make_async_remote_copy(
            src_ref=quant_ref.at[pl.ds(at, block)],
            dst_ref=partner_q.at[pl.ds(at, block)],
            send_sem=swap_send.at[n],
            recv_sem=swap_recv.at[n],
            device_id={"clients": me ^ 1},
        )

    def swap_wait(n):
        swap_copy(n).wait_send()
        at = pl.multiple_of(block_row(*work[n]), 8)
        pltpu.make_async_remote_copy(
            src_ref=partner_q.at[pl.ds(at, block)],
            dst_ref=partner_q.at[pl.ds(at, block)],
            send_sem=swap_send.at[n],
            recv_sem=swap_recv.at[n],
            device_id={"clients": me ^ 1},
        ).wait_recv()

    def pair_row(u, share):
        each = per_block if share else others * per_block
        r = u - (0 if not share else 2 * others * per_block)
        h = (r >= each).astype(jnp.int32)
        r = r - h * each
        k = 0 if share else others - r // per_block
        a = (shares[0] ^ k) * block
        b = half + (shares[1] ^ (2 * k)) * block
        row = jnp.where(h == 1, b, a) + (r % per_block) * unit
        return pl.multiple_of(row, unit)

    early = min(2, len(work))
    pl.semaphore_wait(barrier, peers)
    for n in range(early):
        swap_copy(n).start()
    for h in (1, 0):
        _, keep, give, count, _, _ = plans[h][0][0]
        mask_rows(give, count)
    lane = lax.broadcasted_iota(jnp.int32, (checks, LANES), 1)
    base[...] = (lane + start) * 747796405 + seeds_ref[...]
    tables[1] = jnp.zeros_like(tables[1])
    pieces[1] = jnp.zeros_like(pieces[1])
    for h in (1, 0):
        scatter_copy(h, 0).start()
    for n in range(early, len(work)):
        swap_copy(n).start()
    for h in range(2):
        _, keep, give, count, _, _ = plans[h][0][0]
        mask_rows(keep, count)

    sub = lax.broadcasted_iota(jnp.int32, (8, LANES), 0)
    empty = jnp.zeros((8, LANES), jnp.float32)
    shift = 7 * (sub & 3)
    second = sub >= 4

    def pending(slot, total):
        part = lax.dot_general(
            pieces[slot], tables[slot], (((1,), (1,)), ((), ())), preferred_element_type=jnp.float32
        )
        return reduce_mod(total + part.astype(jnp.int32))

    def fill(slot, row, share):
        for k in range(GROUP):
            at = row + k
            high, low = table_tile(base[...] + at * STRIDE)
            cols = pl.ds(k * LANES, LANES)
            tables[slot, :checks, cols] = high
            tables[slot, checks:, cols] = low
            one = jnp.broadcast_to(quant_ref[pl.ds(at, 1), :], (8, LANES))
            two = jnp.broadcast_to(partner_q[pl.ds(at, 1), :], (8, LANES))
            both = ((jnp.where(second, two, one) >> shift) & 127).astype(jnp.float32)
            if share:
                three = jnp.broadcast_to(agg[pl.ds(at, 1), :], (8, LANES))
                third = jnp.where(second, 0, (three >> shift) & 127).astype(jnp.float32)
            else:
                third = empty
            both = jnp.concatenate([both, third], 0)
            pieces[slot, :, cols] = both.astype(jnp.bfloat16)

    def compute(first, last, share, total):
        def pair(u, total):
            row = pair_row(u, share)
            total = pending(1, total)
            fill(0, row, share)
            total = pending(0, total)
            fill(1, row + GROUP, share)
            return total

        return lax.fori_loop(first, last, pair, total)

    actions = []
    for n in range(bits):
        for h in (1, 0):
            def take(h=h, n=n):
                scatter_copy(h, n).wait()
                add_arrived(h, n)

            def send(h=h, n=n):
                if n < bits - 1:
                    scatter_copy(h, n + 1).start()
                else:
                    gather_copy(h, 0).start()

            actions.append((take, send))
    for n in range(bits):
        for h in (1, 0):
            def take(h=h, n=n):
                gather_wait(h, n)

            def send(h=h, n=n):
                if n < bits - 1:
                    gather_copy(h, n + 1).start()

            actions.append((take, send))

    pairs = rows // 2 // unit
    shared_from = 2 * others * per_block
    early_part = pairs * 11 // 16
    stops = [early_part * (i + 1) // (2 * bits) for i in range(2 * bits)]
    stops += [
        early_part + (pairs - early_part) * (i + 1) // (2 * bits) for i in range(2 * bits)
    ]
    done, swapped = 0, 0
    total = jnp.zeros((16, LANES), jnp.int32)
    for until, (take, send) in zip(stops, actions):
        while swapped * per_block < until:
            swap_wait(swapped)
            swapped += 1
        if done < min(until, shared_from):
            total = compute(done, min(until, shared_from), False, total)
        if max(done, shared_from) < until:
            total = compute(max(done, shared_from), until, True, total)
        done = until
        take()
        send()
    store = pltpu.make_async_copy(agg, agg_out, out_sem)
    store.start()
    total = pending(1, total)

    own_parts[0] = total
    own_copies = []
    for n in range(1, 2 * shards):
        where = {"shard": lax.rem(here + n % shards, shards)} if n % shards else {}
        if n >= shards:
            where["clients"] = me ^ 1
        own_copies.append(
            pltpu.make_async_remote_copy(
                src_ref=own_parts.at[0],
                dst_ref=own_parts.at[n],
                send_sem=own_send.at[n],
                recv_sem=own_recv.at[n],
                device_id=where,
            )
        )
    for copy in own_copies:
        copy.start()
    for copy in own_copies:
        copy.wait()
    mine, theirs = own_parts[0], own_parts[shards]
    for n in range(1, shards):
        mine = mine + own_parts[n]
        theirs = theirs + own_parts[shards + n]
    total = reduce_mod(mine[:8] + pltpu.roll(theirs[:8], 4, 0))
    own_out[...] = total
    diff = reduce_mod(mine[8:]) - total * alive
    diff = jnp.where(diff < 0, diff + modulus, diff)
    diff_parts[0] = diff
    diff_copies = [
        pltpu.make_async_remote_copy(
            src_ref=diff_parts.at[0],
            dst_ref=diff_parts.at[n],
            send_sem=diff_send.at[n],
            recv_sem=diff_recv.at[n],
            device_id={"clients": me ^ n},
        )
        for n in range(1, clients)
    ]
    for copy in diff_copies:
        copy.start()
    for copy in diff_copies:
        copy.wait()
    for n in range(1, clients):
        diff = diff + diff_parts[n]
    diff_out[...] = reduce_mod(diff)
    store.wait()


def aggregate_and_project(quantized, pair_masks, alive_flags, row_seeds, clients, shards):
    length = quantized.shape[1]
    rows = length // LANES
    checks = row_seeds.shape[0]
    bits = clients.bit_length() - 1
    vmem = pl.BlockSpec(memory_space=pltpu.VMEM)
    return pl.pallas_call(
        functools.partial(aggregate_kernel, clients, length),
        in_specs=[pl.BlockSpec(memory_space=pltpu.SMEM), vmem, vmem, vmem],
        out_specs=[pl.BlockSpec(memory_space=pl.ANY), vmem, vmem],
        out_shape=[
            jax.ShapeDtypeStruct((rows, LANES), jnp.int32),
            jax.ShapeDtypeStruct((8, 2 * checks), jnp.int32),
            jax.ShapeDtypeStruct((8, 2 * checks), jnp.int32),
        ],
        scratch_shapes=[
            pltpu.VMEM((rows, LANES), jnp.int32),
            pltpu.VMEM((rows, LANES), jnp.int32),
            pltpu.VMEM((rows, LANES), jnp.int32),
            pltpu.VMEM((checks, LANES), jnp.int32),
            pltpu.VMEM((2, 2 * checks, GROUP * LANES), jnp.bfloat16),
            pltpu.VMEM((2, 16, GROUP * LANES), jnp.bfloat16),
            pltpu.SemaphoreType.DMA((2, 2 * bits)),
            pltpu.SemaphoreType.DMA((2, 2 * bits)),
            pltpu.SemaphoreType.DMA,
            pltpu.VMEM((2 * shards, 16, 2 * checks), jnp.int32),
            pltpu.VMEM((clients, 8, 2 * checks), jnp.int32),
            pltpu.SemaphoreType.DMA((2 * shards,)),
            pltpu.SemaphoreType.DMA((2 * shards,)),
            pltpu.SemaphoreType.DMA((clients,)),
            pltpu.SemaphoreType.DMA((clients,)),
            pltpu.VMEM((rows, LANES), jnp.int32),
            pltpu.SemaphoreType.DMA((clients,)),
            pltpu.SemaphoreType.DMA((clients,)),
        ],
        compiler_params=pltpu.CompilerParams(collective_id=0, has_side_effects=True),
        name="aggregate_and_project",
    )(
        alive_flags,
        row_seeds[:, None],
        quantized.reshape(rows, LANES),
        pair_masks.reshape(rows, LANES),
    )


def checksum(parts):
    checks = parts.shape[1] // 2
    parts = reduce_mod(parts[:, :checks] + parts[:, checks:])
    return reduce_mod(reduce_mod(parts[2] * 128 + parts[1]) * 128 + parts[0])


def body(quantized, pair_masks, alive_flags, row_seeds):
    length = quantized.shape[1]
    clients = lax.axis_size("clients")
    shards = lax.axis_size("shard")
    aggregate, own, diff = aggregate_and_project(
        quantized, pair_masks, alive_flags, row_seeds, clients, shards
    )
    return (aggregate.reshape(length), checksum(own)[None, :], checksum(diff))


def solution(mesh):
    placed = (P("clients", "shard"), P("clients", "shard"), P("clients"), P())
    return jax.shard_map(
        body,
        mesh=mesh,
        in_specs=placed,
        out_specs=(P("shard"), P("clients", None), P()),
        check_vma=False,
    )
```
